256 devices in a mesh: parts: 2 (over z), seq: 128 (over x, y, core).
Axes of the slice: x: 8, y: 8, z: 2, core: 2. Of those that a mesh axis runs over, the one named last changes fastest.
The devices are a block of a 8x8x16 slice.
Arguments:
- token_ids: int32 [4, 4], P(None, 'parts'), parts along dimension 1, may hold values from 0 to 76031
- lengths: int32 [4], P('parts'), parts along dimension 0, may hold values from 24576 to 32768, as said below
- embed_table: bfloat16 [76032, 5120], P('seq'), may hold values from -6 to 6
- attn_gain: bfloat16 [5120], replicated, may hold values from 0.25 to 1.75
- w_qkv: bfloat16 [5120, 7168], P('seq'), may hold values from -0.3125 to 0.3125
- qkv_bias: float32 [7168], replicated, may hold values from -8 to 8
- cache_keys: bfloat16 [4, 32768, 1024], P('parts', 'seq'), parts along dimension 0, may hold values from -300 to 300
- cache_values: bfloat16 [4, 32768, 1024], P('parts', 'seq'), parts along dimension 0, may hold values from -6 to 6
- w_out: bfloat16 [5120, 5120], P(None, 'seq'), may hold values from -0.078125 to 0.078125
- mlp_gain: bfloat16 [5120], replicated, may hold values from 0.25 to 1.75
- w_gate: bfloat16 [5120, 16384], P(None, 'seq'), may hold values from -0.078125 to 0.078125
- w_up: bfloat16 [5120, 16384], P(None, 'seq'), may hold values from -0.078125 to 0.078125
- w_down: bfloat16 [16384, 5120], P('seq'), may hold values from -0.1875 to 0.1875
Outputs:
- attended: bfloat16 [4, 4, 5120], P(None, 'parts'), parts along dimension 1
- layer_out: bfloat16 [4, 4, 5120], P(None, 'parts', 'seq'), parts along dimension 1
The draws below stay inside these ranges and needn't reach their ends.
There are 2 independent parts, one for each index of `parts`. The reference program is written for one: setup_inputs(seed, part) draws one part's arguments, and reference() takes and returns one part's arrays. A program takes and returns all parts, laid end to end along the dimension named above; an argument that names none is the same for every part. Nothing has to cross between parts.
Inputs may be any that keep to these rules, and one draw needn't show every extreme that they name: Cache positions lengths[b] and later are unused; the first prompt fills the whole cache of 32768 positions.
All inputs are finite; a program needn't handle non-finite values.
Results may differ from the reference program's by a relative error of at most 0.017.
The reference program's roundings to bfloat16 on the way (of `normed`, `joint`, `normed_mid` and `hidden`) count: a program that leaves them out, or rounds other values in their place, can miss the bound.
Values may be sent and summed in bfloat16 or wider, within the bound.
No kernel may reach another device: no remote copies, remote signals or barrier semaphores. Data moves between devices by JAX's collectives and lax.ppermute only.
A program may use at most 128 MiB of HBM per device.

```python
import jax
import jax.numpy as jnp
from jax import lax

D = 5120
HEADS = 40
KV_HEADS = 8
HEAD_DIM = 128
FF = 16384
VOCAB = 76032
CTX = 32768
STEPS = 4
SEQS = 2
QD = 5120
KVD = 1024
QKV = 7168


def draw_lengths(key, part):
    drawn = jax.random.randint(jax.random.fold_in(key, 3), (SEQS,), CTX - CTX // 4, CTX + 1, dtype=jnp.int32)
    return drawn.at[0].set(CTX)


def draw_qkv_bias(key, part):
    key_one, key_two, key_three, key_four = jax.random.split(jax.random.fold_in(key, 11), 4)
    direction = jax.random.normal(key_one, (KV_HEADS, HEAD_DIM), jnp.float32)
    strength = jax.random.uniform(key_two, (KV_HEADS, 1), jnp.float32, 1.05, 1.3)
    aligned = direction * strength
    query_noise = 0.5 * jax.random.normal(key_three, (KV_HEADS, HEADS // KV_HEADS, HEAD_DIM), jnp.float32)
    query_part = (aligned[:, None, :] + query_noise).reshape(HEADS * HEAD_DIM)
    key_part = aligned.reshape(KV_HEADS * HEAD_DIM)
    value_part = 0.5 * jax.random.normal(key_four, (KV_HEADS * HEAD_DIM,), jnp.float32)
    joined = jnp.concatenate([query_part, key_part, value_part])
    return jnp.clip(joined, -8.0, 8.0)


def draw_cache_keys(key, part):
    key_one = jax.random.fold_in(jax.random.fold_in(key, 17), 0)
    base = 2.2 * jax.random.normal(key_one, (SEQS, CTX, KV_HEADS, HEAD_DIM), jnp.float32)
    return jnp.clip(base, -300.0, 300.0).reshape(SEQS, CTX, KV_HEADS * HEAD_DIM).astype(jnp.bfloat16)


def touch_ends(entries, key, low, largest):
    dims = entries.shape
    index_at = [jax.random.randint(jax.random.fold_in(key, axis), (), 0, dims[axis]) for axis in range(len(dims))]
    entries = entries.at[tuple(index_at)].set(low)
    longest = dims.index(max(dims))
    index_at[longest] = (index_at[longest] + 1) % dims[longest]
    return entries.at[tuple(index_at)].set(largest)


def spiked(values, rng, source, target, parts, factor):
    def block_of(dim):
        return (jnp.arange(values.shape[dim]) // (values.shape[dim] // parts)).reshape((-1,) + (1,) * (values.ndim - 1 - dim))

    first = jax.random.permutation(rng, parts)[block_of(target)]
    far = (block_of(target) + parts // 2) % parts
    return jnp.where((block_of(source) == first) | (block_of(source) == far), factor * values, values)


def level_of(rng, shape, shards, smallest, top_value):
    level, own = 1.0, jax.random.fold_in(rng, 6)
    for dim, parts in shards:
        steps = jnp.exp(jax.random.uniform(jax.random.fold_in(own, dim), (parts,), jnp.float32, smallest / len(shards), top_value / len(shards)))
        level = level * jnp.repeat(steps, shape[dim] // parts).reshape([-1 if axis == dim else 1 for axis in range(len(shape))])
    return level


def gaussian(key, shape, spread, most, pieces=(), held_as=jnp.bfloat16):
    values = jax.random.normal(key, shape, jnp.float32) * spread
    if len(pieces) > 0:
        values = level_of(key, shape, pieces, -0.22, 0.18) * values
    return jnp.clip(values, min=-most, max=most).astype(held_as)


def heavy_noise(own_key, shape, spread, most, shards, heavy, held_as=jnp.bfloat16):
    entries = spread * jax.random.normal(own_key, shape, jnp.float32)
    if shards:
        entries = entries * level_of(own_key, shape, shards, -0.22, 0.18)
    return jnp.clip(spiked(entries, jax.random.fold_in(own_key, 3), *heavy), -most, most).astype(held_as)


def setup_inputs(seed: int = 0, part: int = 0) -> dict:
    streams_of = jax.random.split(jax.random.key(seed), 14)
    part_keys = jax.random.split(jax.random.fold_in(streams_of[13], part), 14)
    token_ids = touch_ends(jax.random.randint(part_keys[0], (STEPS, SEQS), 0, VOCAB), jax.random.fold_in(part_keys[0], 1), 0, VOCAB - 1).astype(jnp.int32)
    lengths = draw_lengths(jax.random.fold_in(jax.random.fold_in(streams_of[13], part), 71), part)
    embed_table = gaussian(streams_of[2], (VOCAB, D), 0.5, 6.0, ((0, 128),))
    attn_gain = jnp.clip(1.0 + 0.15 * jax.random.normal(streams_of[3], (D,), jnp.float32), 0.25, 1.75).astype(jnp.bfloat16)
    w_qkv = heavy_noise(streams_of[4], (D, QKV), D ** -0.5, 0.3125, ((0, 128),), (0, 1, 128, 5.5))
    qkv_bias = draw_qkv_bias(jax.random.fold_in(streams_of[13], 71), part)
    cache_keys = draw_cache_keys(jax.random.fold_in(jax.random.fold_in(streams_of[13], part), 71), part)
    cache_values = gaussian(part_keys[7], (SEQS, CTX, KVD), 1.0, 6.0, ((1, 128),))
    w_out = gaussian(streams_of[8], (QD, D), QD ** -0.5, 0.078125, ((1, 128),))
    mlp_gain = jnp.clip(1.0 + 0.15 * jax.random.normal(streams_of[9], (D,), jnp.float32), 0.25, 1.75).astype(jnp.bfloat16)
    w_gate = gaussian(streams_of[10], (D, FF), D ** -0.5, 0.078125, ((1, 128),))
    w_up = gaussian(streams_of[11], (D, FF), D ** -0.5, 0.078125, ((1, 128),))
    w_down = heavy_noise(streams_of[12], (FF, D), FF ** -0.5, 0.1875, ((0, 128),), (0, 1, 128, 5.5))
    return {"token_ids": token_ids, "lengths": lengths, "embed_table": embed_table, "attn_gain": attn_gain, "w_qkv": w_qkv, "qkv_bias": qkv_bias, "cache_keys": cache_keys, "cache_values": cache_values, "w_out": w_out, "mlp_gain": mlp_gain, "w_gate": w_gate, "w_up": w_up, "w_down": w_down}


NORM_EPS = 1e-06
ROPE_BASE = 1000000.0
MASKED = -1e+30

def rms_normalize(rows, gain):
    mean_square = lax.optimization_barrier(jnp.mean(rows * rows, axis=-1, keepdims=True))
    return (rows * lax.rsqrt(mean_square + NORM_EPS) * gain.astype(jnp.float32)).astype(jnp.bfloat16)

def rotate(vectors, positions):
    half_dim = vectors.shape[-1] // 2
    frequency = ROPE_BASE ** (-2.0 * jnp.arange(half_dim, dtype=jnp.float32) / vectors.shape[-1])
    angles = positions.astype(jnp.float32)[..., None, None] * frequency
    cosine = jnp.cos(angles)
    sine_part = jnp.sin(angles)
    widened = vectors.astype(jnp.float32)
    first_half = widened[..., :half_dim]
    second = widened[..., half_dim:]
    joined = jnp.concatenate([first_half * cosine - second * sine_part, second * cosine + first_half * sine_part], axis=-1)
    return joined.astype(jnp.bfloat16)

def attend_one(query_rows, key_rows, value_rows, cached_keys, cached_values, length):
    all_keys = jnp.concatenate([cached_keys.reshape(CTX, KV_HEADS, HEAD_DIM), key_rows], axis=0).astype(jnp.float32)
    all_values = jnp.concatenate([cached_values.reshape(CTX, KV_HEADS, HEAD_DIM), value_rows], axis=0).astype(jnp.float32)
    grouped = query_rows.reshape(STEPS, KV_HEADS, HEADS // KV_HEADS, HEAD_DIM).astype(jnp.float32)
    scores = jnp.einsum('skgd,pkd->kgsp', grouped, all_keys) * HEAD_DIM ** (-0.5)
    places = jnp.arange(CTX + STEPS, dtype=jnp.int32)
    step_index = jnp.arange(STEPS, dtype=jnp.int32)
    cache_valid = places[None, :] < length
    new_valid = places[None, :] - CTX <= step_index[:, None]
    valid = jnp.where(places[None, :] < CTX, cache_valid, new_valid)
    masked = jnp.where(valid, scores, MASKED)
    top_score = lax.optimization_barrier(jnp.max(masked, axis=-1, keepdims=True))
    weights = jnp.where(valid, jnp.exp(masked - top_score), 0.0)
    total = lax.optimization_barrier(jnp.sum(weights, axis=-1))
    rounded = lax.optimization_barrier(weights.astype(jnp.bfloat16)).astype(jnp.float32)
    summed = jnp.einsum('kgsp,pkd->kgsd', rounded, all_values)
    result = summed / total[..., None]
    result = jnp.transpose(result, (2, 0, 1, 3))
    return result.reshape(STEPS, HEADS * HEAD_DIM).astype(jnp.bfloat16)

def reference(token_ids, lengths, embed_table, attn_gain, w_qkv, qkv_bias, cache_keys, cache_values, w_out, mlp_gain, w_gate, w_up, w_down):
    query_width = HEADS * HEAD_DIM
    key_width = KV_HEADS * HEAD_DIM
    stream = embed_table[token_ids].astype(jnp.float32)
    normed = rms_normalize(stream, attn_gain)
    joint = jnp.dot(normed.reshape(-1, D), w_qkv, preferred_element_type=jnp.float32) + qkv_bias.astype(jnp.float32)
    joint = joint.astype(jnp.bfloat16).reshape(STEPS, SEQS, -1)
    query_part = joint[..., :query_width].reshape(STEPS, SEQS, HEADS, HEAD_DIM)
    key_part = joint[..., query_width:query_width + key_width].reshape(STEPS, SEQS, KV_HEADS, HEAD_DIM)
    value_part = joint[..., query_width + key_width:].reshape(STEPS, SEQS, KV_HEADS, HEAD_DIM)
    positions = lengths[None, :] + jnp.arange(STEPS, dtype=jnp.int32)[:, None]
    queries = rotate(query_part, positions)
    new_keys = rotate(key_part, positions)
    outputs = []
    for seq_index in range(SEQS):
        outputs.append(attend_one(queries[:, seq_index], new_keys[:, seq_index], value_part[:, seq_index], cache_keys[seq_index], cache_values[seq_index], lengths[seq_index]))
    attended = jnp.stack(outputs, axis=1)
    projected = jnp.dot(attended.reshape(-1, query_width), w_out, preferred_element_type=jnp.float32)
    mid = stream + projected.reshape(STEPS, SEQS, D)
    normed_mid = rms_normalize(mid, mlp_gain).reshape(-1, D)
    gate = jnp.dot(normed_mid, w_gate, preferred_element_type=jnp.float32)
    upper = jnp.dot(normed_mid, w_up, preferred_element_type=jnp.float32)
    hidden = (jax.nn.silu(gate) * upper).astype(jnp.bfloat16)
    down = jnp.dot(hidden, w_down, preferred_element_type=jnp.float32).reshape(STEPS, SEQS, D)
    layer_out = (mid + down).astype(jnp.bfloat16)
    return (attended, layer_out)
```

```python
import math

import jax
import jax.numpy as jnp
from jax import lax
from jax.sharding import Mesh
from jax.sharding import PartitionSpec as P

HEADS = 40
KV_HEADS = 8
HEAD_DIM = 128
SEQ = ("seq_0", "seq_1", "seq_2")


NORM_EPS = 1e-06
ROPE_BASE = 1000000.0
MASKED = -1e30
F32 = jnp.float32
BF16 = jnp.bfloat16


def swap(parts):
    return lax.all_to_all(parts, SEQ, 0, 0)


def share(piece):
    members = lax.axis_size(SEQ)
    return swap(jnp.broadcast_to(piece[None], (members, *piece.shape)))


def pieces_of(value, count):
    found, rest = [], value
    for _ in range(count):
        part = lax.reduce_precision(rest, 8, 7)
        found.append(part.astype(BF16))
        rest = rest - part
    return found


def rotate(vectors, positions):
    half_dim = vectors.shape[-1] // 2
    frequency = ROPE_BASE ** (-2.0 * jnp.arange(half_dim, dtype=F32) / vectors.shape[-1])
    angles = positions.astype(F32)[..., None, None] * frequency
    cosine = jnp.cos(angles)
    sine_part = jnp.sin(angles)
    widened = vectors.astype(F32)
    first_half = widened[..., :half_dim]
    second = widened[..., half_dim:]
    joined = jnp.concatenate(
        [first_half * cosine - second * sine_part, second * cosine + first_half * sine_part],
        axis=-1,
    )
    return joined.astype(BF16)


def split_columns(array, members):
    rows, width = array.shape
    return array.reshape(rows, members, width // members).transpose(1, 0, 2)


def join_columns(parts):
    members, rows, width = parts.shape
    return parts.transpose(1, 0, 2).reshape(rows, members * width)


def body(
    token_ids,
    lengths,
    embed_table,
    attn_gain,
    w_qkv,
    qkv_bias,
    cache_keys,
    cache_values,
    w_out,
    mlp_gain,
    w_gate,
    w_up,
    w_down,
):
    rank = lax.axis_index(SEQ)
    members = lax.axis_size(SEQ)
    steps, batch = token_ids.shape
    tokens = steps * batch
    model_width = embed_table.shape[1]
    vocab_rows = embed_table.shape[0]
    query_width = HEADS * HEAD_DIM
    key_width = KV_HEADS * HEAD_DIM
    group_size = HEADS // KV_HEADS
    half = HEAD_DIM // 2

    local_ids = token_ids.reshape(-1) - rank * vocab_rows
    one_hot = (local_ids[:, None] == jnp.arange(vocab_rows)[None, :]).astype(BF16)
    rows = jnp.dot(one_hot, embed_table, preferred_element_type=F32)
    square = jnp.mean(rows * rows, axis=-1)
    tail = jnp.stack(pieces_of(square, 3), axis=-1)
    sent = jnp.concatenate(
        [
            split_columns(rows.astype(BF16), members),
            jnp.broadcast_to(tail[None], (members, *tail.shape)),
        ],
        axis=-1,
    )
    got = jnp.sum(swap(sent).astype(F32), axis=0)
    features = w_qkv.shape[0]
    stream = got[:, :features]
    square = jnp.sum(got[:, features:], axis=-1, keepdims=True)
    gain = lax.dynamic_slice_in_dim(attn_gain, rank * features, features, 0)
    normed = (stream * lax.rsqrt(square + NORM_EPS) * gain.astype(F32)).astype(BF16)

    joint_partial = jnp.dot(normed, w_qkv, preferred_element_type=F32)
    columns = w_qkv.shape[1] // members
    joint_sum = jnp.sum(
        swap(split_columns(joint_partial.astype(BF16), members)).astype(F32), axis=0
    )
    bias = lax.dynamic_slice_in_dim(qkv_bias, rank * columns, columns, 0)
    joint = join_columns(share((joint_sum + bias).astype(BF16))).reshape(steps, batch, -1)

    query_part = joint[..., :query_width].reshape(steps, batch, HEADS, HEAD_DIM)
    key_part = joint[..., query_width : query_width + key_width].reshape(
        steps, batch, KV_HEADS, HEAD_DIM
    )
    value_part = joint[..., query_width + key_width :].reshape(
        steps, batch, KV_HEADS, HEAD_DIM
    )
    positions = lengths[None, :] + jnp.arange(steps, dtype=jnp.int32)[:, None]
    queries = rotate(query_part, positions)
    new_keys = rotate(key_part, positions)
    grouped = queries.reshape(steps, batch, KV_HEADS, group_size, HEAD_DIM)
    score_scale = 1.0 / math.sqrt(HEAD_DIM)

    local_len = cache_keys.shape[1]
    key_blocks = cache_keys.reshape(batch, local_len, KV_HEADS, HEAD_DIM)
    value_blocks = cache_values.reshape(batch, local_len, KV_HEADS, HEAD_DIM)
    scores = (
        jnp.einsum("sbkgd,bpkd->bksgp", grouped, key_blocks, preferred_element_type=F32)
        * score_scale
    )
    places = rank * local_len + jnp.arange(local_len, dtype=jnp.int32)
    valid = (places[None, :] < lengths[:, None])[:, None, None, None, :]
    new_scores = (
        jnp.einsum("sbkgd,tbkd->bksgt", grouped, new_keys, preferred_element_type=F32)
        * score_scale
    )
    step_index = jnp.arange(steps, dtype=jnp.int32)
    new_valid = ((step_index[:, None] >= step_index[None, :]) & (rank == 0))[None, None, :, None, :]
    masked = jnp.where(valid, scores, MASKED)
    new_masked = jnp.where(new_valid, new_scores, MASKED)
    top = jnp.maximum(jnp.max(masked, axis=-1), jnp.max(new_masked, axis=-1))
    weights = jnp.where(valid, jnp.exp(masked - top[..., None]), 0.0)
    new_weights = jnp.where(new_valid, jnp.exp(new_masked - top[..., None]), 0.0)
    total = jnp.sum(weights, axis=-1) + jnp.sum(new_weights, axis=-1)
    summed = jnp.einsum(
        "bksgp,bpkd->bksgd", weights.astype(BF16), value_blocks, preferred_element_type=F32
    ) + jnp.einsum(
        "bksgt,tbkd->bksgd", new_weights.astype(BF16), value_part, preferred_element_type=F32
    )
    groups = batch * KV_HEADS * steps
    summed = summed.reshape(groups, group_size, 2, half).transpose(0, 2, 1, 3)
    extra = jnp.stack(pieces_of(top, 3) + pieces_of(total, 3), axis=-1)
    extra = jnp.broadcast_to(
        extra.reshape(groups, 1, group_size, 6), (groups, 2, group_size, 6)
    )
    sent = jnp.concatenate([summed.astype(BF16), extra], axis=-1)
    got = swap(sent.reshape(members, group_size, half + 6)).astype(F32)
    tops = jnp.sum(got[..., half : half + 3], axis=-1, keepdims=True)
    totals = jnp.sum(got[..., half + 3 :], axis=-1, keepdims=True)
    scale = jnp.exp(tops - jnp.max(tops, axis=0, keepdims=True))
    merged = jnp.sum(got[..., :half] * scale, axis=0) / jnp.sum(totals * scale, axis=0)
    attended = share(merged.astype(BF16))
    attended = attended.reshape(batch, KV_HEADS, steps, 2, group_size, half)
    attended = attended.transpose(2, 0, 1, 4, 3, 5).reshape(steps, batch, query_width)

    projected = jnp.dot(attended.reshape(tokens, query_width), w_out, preferred_element_type=F32)
    mid = stream + projected
    width = w_out.shape[1]
    pair = share(jnp.concatenate(pieces_of(mid, 2), axis=-1)).astype(F32)
    mid_rows = pair[..., :width] + pair[..., width:]
    mean_square = jnp.sum(mid_rows * mid_rows, axis=(0, 2)) / model_width
    normed_mid = (
        mid_rows
        * lax.rsqrt(mean_square + NORM_EPS)[None, :, None]
        * mlp_gain.astype(F32).reshape(members, 1, width)
    ).astype(BF16)
    flat = join_columns(normed_mid)

    gate = jnp.dot(flat, w_gate, preferred_element_type=F32)
    upper = jnp.dot(flat, w_up, preferred_element_type=F32)
    hidden = (jax.nn.silu(gate) * upper).astype(BF16)
    down = jnp.dot(hidden, w_down, preferred_element_type=F32)
    summed = jnp.sum(swap(split_columns(down.astype(BF16), members)).astype(F32), axis=0)
    layer_out = (mid + summed).astype(BF16).reshape(steps, batch, width)
    return (attended, layer_out)


def solution(mesh):
    finer = Mesh(
        mesh.devices.reshape(mesh.shape["parts"], 8, 8, 2), ("parts", "seq_0", "seq_1", "seq_2")
    )
    return jax.shard_map(
        body,
        mesh=finer,
        in_specs=(
            P(None, "parts"),
            P("parts"),
            P(SEQ, None),
            P(),
            P(SEQ, None),
            P(),
            P("parts", SEQ, None),
            P("parts", SEQ, None),
            P(None, SEQ),
            P(),
            P(None, SEQ),
            P(None, SEQ),
            P(SEQ, None),
        ),
        out_specs=(P(None, "parts", None), P(None, "parts", SEQ)),
        check_vma=False,
    )
```

```python
import functools
import math

import jax
import jax.numpy as jnp
from jax import lax
from jax.experimental import pallas as pl
from jax.experimental.pallas import tpu as pltpu
from jax.sharding import Mesh
from jax.sharding import PartitionSpec as P

HEADS = 40
KV_HEADS = 8
HEAD_DIM = 128
SEQ = ("seq_0", "seq_1", "seq_2")
CHIPS = ("seq_0", "seq_1")
CORE = "seq_2"

NORM_EPS = 1e-06
ROPE_BASE = 1000000.0
MASKED = -1e30
F32 = jnp.float32
BF16 = jnp.bfloat16
HALF = HEAD_DIM // 2
GROUP = HEADS // KV_HEADS
KV_HALF = KV_HEADS // 2
Q_HALF = HEADS // 2
BLOCKS = Q_HALF + 2 * KV_HALF

WHOLE = pl.BlockSpec(memory_space=pltpu.VMEM)
SCALARS = pl.BlockSpec(memory_space=pltpu.SMEM)


def kernel_call(body, out_shape, in_specs, scratch=(), name=None):
    many = isinstance(out_shape, (tuple, list))
    return pl.pallas_call(
        body,
        out_shape=out_shape,
        in_specs=in_specs,
        out_specs=[WHOLE] * len(out_shape) if many else WHOLE,
        scratch_shapes=list(scratch),
        name=name,
    )


def swap(parts):
    return lax.all_to_all(parts, CHIPS, 0, 0)


def partner(array):
    return lax.ppermute(array, CORE, [(0, 1), (1, 0)])


def lanes(shape):
    return lax.broadcasted_iota(jnp.int32, shape, len(shape) - 1)


def pick_kernel(vocab_rows, ids, *refs):
    tokens = len(refs) - 2
    blocks, out, rows = refs[:tokens], refs[tokens], refs[tokens + 1]
    chips, _, lane_count = out.shape
    model_width = rows.shape[1]
    width = model_width // chips
    for t in range(tokens):
        place = ids[t]
        inside = (place >= 0) & (place < vocab_rows)
        row = jnp.where(inside, place & 7, -1)
        block = blocks[t][...].astype(F32)
        at = lax.broadcasted_iota(jnp.int32, block.shape, 0)
        rows[t : t + 1, :] = jnp.sum(jnp.where(at == row, block, 0.0), axis=0, keepdims=True)
    values = rows[...]
    square = jnp.mean(values * values, axis=-1, keepdims=True)
    tail = jnp.broadcast_to(square, (tokens, lane_count - width))
    for j in range(chips):
        out[j, :, :width] = rows[:, j * width : (j + 1) * width]
        out[j, :, width:] = tail


def pick(ids, table, chips):
    vocab_rows, model_width = table.shape
    tokens = ids.shape[0]

    def block_of(t, _, places):
        return (jnp.clip(places[t], 0, vocab_rows - 1) // 8, 0)

    return pl.pallas_call(
        functools.partial(pick_kernel, vocab_rows),
        out_shape=jax.ShapeDtypeStruct((chips, tokens, 128), F32),
        grid_spec=pltpu.PrefetchScalarGridSpec(
            num_scalar_prefetch=1,
            grid=(1,),
            in_specs=[
                pl.BlockSpec((8, model_width), functools.partial(block_of, t))
                for t in range(tokens)
            ],
            out_specs=pl.BlockSpec((chips, tokens, 128), lambda _, places: (0, 0, 0)),
            scratch_shapes=[pltpu.VMEM((tokens, model_width), F32)],
        ),
        name="pick",
    )(ids, *([table] * tokens))


def joint_kernel(core, own, other, gain, weights, out, stream_out):
    c = core[0]
    width = gain.shape[1]
    both = own[...] + other[...]
    stream = both[:, :width]
    square = both[:, width : width + 1]
    normed = (stream * lax.rsqrt(square + NORM_EPS) * gain[...]).astype(BF16)
    stream_out[...] = stream
    at = 0
    for first, count in ((0, Q_HALF), (HEADS, KV_HALF), (HEADS + KV_HEADS, KV_HALF)):
        start = pl.multiple_of((first + count * c) * HEAD_DIM, HEAD_DIM)
        product = jnp.dot(
            normed, weights[:, pl.ds(start, count * HEAD_DIM)], preferred_element_type=F32
        )
        for i in range(count):
            out[at + i] = product[:, i * HEAD_DIM : (i + 1) * HEAD_DIM]
        at += count
    out[at:] = jnp.zeros((out.shape[0] - at, *out.shape[1:]), F32)


def rotate_kernel(place, got, bias, cosine, sine, out):
    total = jnp.sum(got[...], axis=0) + bias[pl.ds(place[0], 1), :]
    joint = total.astype(BF16).astype(F32)
    turned = joint * cosine[...] + pltpu.roll(joint, HALF, 1) * sine[...]
    result = jnp.where(place[1] > 0, turned, joint).astype(BF16)
    out[...] = jnp.broadcast_to(result[None], out.shape)


def attend_kernel(info, heads, keys, other_keys, values, other_values, out):
    tokens = heads.shape[1]
    batch, local_len, _ = keys.shape
    rows = GROUP * tokens
    score_scale = 1.0 / math.sqrt(HEAD_DIM)
    token = lax.broadcasted_iota(jnp.int32, (rows, 1), 0) % tokens
    prompt = token % batch
    spot = lax.broadcasted_iota(jnp.int32, (1, local_len), 1)
    fresh = lax.broadcasted_iota(jnp.int32, (1, tokens), 1)
    fresh_valid = (fresh % batch == prompt) & (fresh <= token) & (info[3] > 0)
    contract = (((1,), (1,)), ((), ()))
    lane = lanes((tokens, HEAD_DIM))
    valid = [
        [(spot + info[1 + side] < info[4 + b]) & (prompt == b) for b in range(batch)]
        for side in range(2)
    ]
    for h in range(KV_HALF):
        columns = slice(h * HEAD_DIM, (h + 1) * HEAD_DIM)
        query = heads[h * GROUP : (h + 1) * GROUP].astype(F32).reshape(rows, HEAD_DIM).astype(BF16)
        scores, kept, matching = [], [], []
        for side, (k_ref, v_ref) in enumerate(((keys, values), (other_keys, other_values))):
            for b in range(batch):
                score = lax.dot_general(
                    query, k_ref[b, :, columns], contract, preferred_element_type=F32
                )
                scores.append(jnp.where(valid[side][b], score * score_scale, MASKED))
                kept.append(valid[side][b])
                matching.append(v_ref[b, :, columns])
        score = lax.dot_general(
            query, heads[Q_HALF + h], contract, preferred_element_type=F32
        )
        scores.append(jnp.where(fresh_valid, score * score_scale, MASKED))
        kept.append(fresh_valid)
        matching.append(heads[Q_HALF + KV_HALF + h])
        top = functools.reduce(
            jnp.maximum, [jnp.max(s, axis=-1, keepdims=True) for s in scores]
        )
        total = jnp.zeros((rows, 1), F32)
        summed = jnp.zeros((rows, HEAD_DIM), F32)
        for s, keep, value in zip(scores, kept, matching):
            weight = jnp.where(keep, jnp.exp(s - top), 0.0)
            total += jnp.sum(weight, axis=-1, keepdims=True)
            summed += jnp.dot(weight.astype(BF16), value, preferred_element_type=F32)
        for g in range(GROUP):
            part = slice(g * tokens, (g + 1) * tokens)
            extra = jnp.where(lane == HALF, top[part], total[part])
            both = summed[part]
            at = 2 * (h * GROUP + g)
            out[at] = jnp.where(lane < HALF, both, extra)
            out[at + 1] = jnp.where(lane < HALF, pltpu.roll(both, HALF, 1), extra)
    used = 2 * Q_HALF
    out[used:] = jnp.zeros((out.shape[0] - used, *out.shape[1:]), F32)


def attend(info, heads, keys, other_keys, values, other_values):
    batch, local_len, key_width = keys.shape
    cut = key_width // 2
    whole = pl.BlockSpec(heads.shape, lambda _, i: (0, 0, 0))
    mine = pl.BlockSpec((batch, local_len, cut), lambda _, i: (0, 0, i[0]))
    return pl.pallas_call(
        attend_kernel,
        out_shape=jax.ShapeDtypeStruct(heads.shape, F32),
        grid_spec=pltpu.PrefetchScalarGridSpec(
            num_scalar_prefetch=1,
            grid=(1,),
            in_specs=[whole, mine, mine, mine, mine],
            out_specs=whole,
        ),
        name="attend",
    )(info, heads, keys, other_keys, values, other_values)


def merge_kernel(got, out):
    parts = got[...]
    tops = parts[:, :, HALF : HALF + 1]
    scale = jnp.exp(tops - jnp.max(tops, axis=0, keepdims=True))
    merged = jnp.sum(parts * scale, axis=0)
    total = merged[:, HALF + 1 : HALF + 2]
    result = (merged / jnp.where(total > 0.0, total, 1.0)).astype(BF16)
    out[...] = jnp.broadcast_to(result[None], out.shape)


def project_kernel(core, own, other, weights, stream, attended, mid_out, out):
    c = core[0]
    tokens, width = stream.shape
    lane = lanes((tokens, HEAD_DIM))
    for pieces, start in ((own, c * Q_HALF), (other, (1 - c) * Q_HALF)):
        for i in range(Q_HALF):
            low = pieces[2 * i].astype(F32)
            high = pltpu.roll(pieces[2 * i + 1].astype(F32), HALF, 1)
            column = pl.multiple_of((start + i) * HEAD_DIM, HEAD_DIM)
            attended[:, pl.ds(column, HEAD_DIM)] = jnp.where(lane < HALF, low, high).astype(BF16)
    mid = stream[...] + lax.dot_general(
        attended[...], weights[...], (((1,), (1,)), ((), ())), preferred_element_type=F32
    )
    mid_out[...] = mid
    padded = jnp.concatenate([mid, jnp.zeros((tokens, HEAD_DIM - width), F32)], axis=1)
    out[...] = jnp.broadcast_to(padded[None], out.shape)


def mlp_kernel(got, gain, w_gate, w_up, w_down, out, flat):
    chips, tokens, lane_count = got.shape
    model_width = flat.shape[1]
    width = model_width // chips
    parts = got[...]
    square = jnp.sum(jnp.sum(parts * parts, axis=0), axis=-1, keepdims=True) / model_width
    for j in range(chips):
        flat[:, j * width : (j + 1) * width] = got[j, :, :width]
    normed = (flat[...] * lax.rsqrt(square + NORM_EPS) * gain[...]).astype(BF16)
    gate = jnp.dot(normed, w_gate[...], preferred_element_type=F32)
    upper = jnp.dot(normed, w_up[...], preferred_element_type=F32)
    hidden = (gate / (1.0 + jnp.exp(-gate)) * upper).astype(BF16)
    flat[...] = jnp.dot(hidden, w_down[...], preferred_element_type=F32)
    tail = jnp.zeros((tokens, lane_count - width), F32)
    for j in range(chips):
        out[j, :, :width] = flat[:, j * width : (j + 1) * width]
        out[j, :, width:] = tail


def body(
    token_ids,
    lengths,
    embed_table,
    attn_gain,
    w_qkv,
    qkv_bias,
    cache_keys,
    cache_values,
    w_out,
    mlp_gain,
    w_gate,
    w_up,
    w_down,
):
    c = lax.axis_index(CORE)
    j = lax.axis_index(CHIPS)
    rank = lax.axis_index(SEQ)
    chips = lax.axis_size(CHIPS)
    steps, batch = token_ids.shape
    tokens = steps * batch
    vocab_rows, model_width = embed_table.shape
    local_len = cache_keys.shape[1]
    features = w_qkv.shape[0]
    width = 2 * features
    core = c.reshape(1)
    tile = (chips, tokens, HEAD_DIM)

    other_qkv = partner(w_qkv)
    other_keys = partner(cache_keys)
    other_values = partner(cache_values)
    own_out = w_out.T
    other_out = partner(own_out)
    first = c == 0
    qkv_rows = jnp.concatenate(
        [jnp.where(first, w_qkv, other_qkv), jnp.where(first, other_qkv, w_qkv)], axis=0
    )
    out_rows = jnp.concatenate(
        [jnp.where(first, own_out, other_out), jnp.where(first, other_out, own_out)], axis=0
    )

    local_ids = token_ids.reshape(-1) - rank * vocab_rows
    got = jnp.sum(swap(pick(local_ids, embed_table, chips)), axis=0)
    gain = lax.dynamic_slice_in_dim(attn_gain, j * width, width, 0).astype(F32)[None]
    sent, stream = kernel_call(
        joint_kernel,
        (jax.ShapeDtypeStruct(tile, F32), jax.ShapeDtypeStruct((tokens, width), F32)),
        [SCALARS] + [WHOLE] * 4,
        name="joint",
    )(core, got, partner(got), gain, qkv_rows)

    positions = (lengths[None, :] + jnp.arange(steps, dtype=jnp.int32)[:, None]).reshape(-1)
    frequency = ROPE_BASE ** (-2.0 * jnp.arange(HALF, dtype=F32) / HEAD_DIM)
    angles = positions.astype(F32)[:, None] * frequency
    cosine = jnp.cos(angles)
    sine = jnp.sin(angles)
    cosine = jnp.concatenate([cosine, cosine], axis=1)
    sine = jnp.concatenate([-sine, sine], axis=1)
    head = jnp.where(
        j < Q_HALF,
        Q_HALF * c + j,
        jnp.where(
            j < Q_HALF + KV_HALF,
            HEADS + KV_HALF * c + (j - Q_HALF),
            HEADS + KV_HEADS + KV_HALF * c + (j - Q_HALF - KV_HALF),
        ),
    )
    head = jnp.where(j < BLOCKS, head, 0)
    place = jnp.stack([head, (j < Q_HALF + KV_HALF).astype(jnp.int32)])
    heads = kernel_call(
        rotate_kernel,
        jax.ShapeDtypeStruct(tile, BF16),
        [SCALARS] + [WHOLE] * 4,
        name="rotate",
    )(place, swap(sent), qkv_bias.reshape(-1, HEAD_DIM), cosine, sine)
    heads = swap(heads)

    info = jnp.stack(
        [
            c,
            rank * local_len,
            (rank + 1 - 2 * c) * local_len,
            (j == 0).astype(jnp.int32),
            *[lengths[b] for b in range(batch)],
        ]
    )
    partial = attend(info, heads, cache_keys, other_keys, cache_values, other_values)
    merged = kernel_call(merge_kernel, jax.ShapeDtypeStruct(tile, BF16), [WHOLE], name="merge")(
        swap(partial)
    )
    pieces = swap(merged)

    attended, mid, sent = kernel_call(
        project_kernel,
        (
            jax.ShapeDtypeStruct((tokens, HEADS * HEAD_DIM), BF16),
            jax.ShapeDtypeStruct((tokens, width), F32),
            jax.ShapeDtypeStruct(tile, F32),
        ),
        [SCALARS] + [WHOLE] * 4,
        name="project",
    )(core, pieces, partner(pieces), out_rows, stream)

    down = kernel_call(
        mlp_kernel,
        jax.ShapeDtypeStruct(tile, F32),
        [WHOLE] * 5,
        [pltpu.VMEM((tokens, model_width), F32)],
        name="mlp",
    )(swap(sent), mlp_gain.astype(F32)[None], w_gate, w_up, w_down)
    summed = jnp.sum(swap(down), axis=0)
    summed = mid + (summed + partner(summed))[:, :width]
    mine = jnp.where(first, summed[:, :features], summed[:, features:])
    layer_out = mine.astype(BF16).reshape(steps, batch, features)
    return (attended.reshape(steps, batch, -1), layer_out)


def solution(mesh):
    finer = Mesh(
        mesh.devices.reshape(mesh.shape["parts"], 8, 8, 2), ("parts", "seq_0", "seq_1", "seq_2")
    )
    return jax.shard_map(
        body,
        mesh=finer,
        in_specs=(
            P(None, "parts"),
            P("parts"),
            P(SEQ, None),
            P(),
            P(SEQ, None),
            P(),
            P("parts", SEQ, None),
            P("parts", SEQ, None),
            P(None, SEQ),
            P(),
            P(None, SEQ),
            P(None, SEQ),
            P(SEQ, None),
        ),
        out_specs=(P(None, "parts", None), P(None, "parts", SEQ)),
        check_vma=False,
    )
```

```python
import functools
import math

import jax
import jax.numpy as jnp
from jax import lax
from jax.experimental import pallas as pl
from jax.experimental.pallas import tpu as pltpu
from jax.sharding import Mesh
from jax.sharding import PartitionSpec as P

HEADS = 40
KV_HEADS = 8
HEAD_DIM = 128
SEQ = ("seq_0", "seq_1", "seq_2")
CHIPS = ("seq_0", "seq_1")
CORE = "seq_2"

NORM_EPS = 1e-06
ROPE_BASE = 1000000.0
MASKED = -1e30
F32 = jnp.float32
BF16 = jnp.bfloat16
HALF = HEAD_DIM // 2
GROUP = HEADS // KV_HEADS
KV_HALF = KV_HEADS // 2
Q_HALF = HEADS // 2
BLOCKS = Q_HALF + 2 * KV_HALF

WHOLE = pl.BlockSpec(memory_space=pltpu.VMEM)
SCALARS = pl.BlockSpec(memory_space=pltpu.SMEM)
STAYS = pl.BlockSpec(memory_space=pltpu.HBM)


def grant(mebibytes):
    return pltpu.CompilerParams(vmem_limit_bytes=mebibytes * 1024 * 1024)


def kernel_call(body, out_shape, in_specs, scratch=(), name=None, room=12):
    many = isinstance(out_shape, (tuple, list))
    return pl.pallas_call(
        body,
        out_shape=out_shape,
        in_specs=in_specs,
        out_specs=[WHOLE] * len(out_shape) if many else WHOLE,
        scratch_shapes=list(scratch),
        compiler_params=grant(room),
        name=name,
    )


def swap(parts):
    return lax.all_to_all(parts, CHIPS, 0, 0)


def partner(array):
    return lax.ppermute(array, CORE, [(0, 1), (1, 0)])


def lanes(shape):
    return lax.broadcasted_iota(jnp.int32, shape, len(shape) - 1)


def in_pieces(value):
    high = value.astype(BF16).astype(F32)
    rest = value - high
    middle = rest.astype(BF16).astype(F32)
    return high, middle, rest - middle


def own_first(core, left, right):
    return jnp.where(core == 0, left, right), jnp.where(core == 0, right, left)


def pick_kernel(vocab_rows, rank, ids, *refs):
    tokens = len(refs) - 2
    batch = ids.shape[0]
    blocks, out, rows = refs[:tokens], refs[tokens], refs[tokens + 1]
    chips, _, lane_count = out.shape
    model_width = rows.shape[1]
    width = model_width // chips
    for t in range(tokens):
        place = ids[t % batch, t // batch] - rank[0] * vocab_rows
        inside = (place >= 0) & (place < vocab_rows)
        row = jnp.where(inside, place & 7, -1)
        block = blocks[t][...].astype(F32)
        at = lax.broadcasted_iota(jnp.int32, block.shape, 0)
        rows[t : t + 1, :] = jnp.sum(jnp.where(at == row, block, 0.0), axis=0, keepdims=True)
    values = rows[...]
    square = in_pieces(jnp.mean(values * values, axis=-1, keepdims=True))
    lane = lanes((tokens, lane_count - width))
    tail = jnp.zeros(lane.shape, F32)
    for i, piece in enumerate(square):
        tail = jnp.where(lane == i, piece, tail)
    for j in range(chips):
        both = jnp.concatenate([rows[:, j * width : (j + 1) * width], tail], axis=1)
        out[j] = both.astype(BF16)


def pick(rank, ids, table, chips):
    vocab_rows, model_width = table.shape
    batch, steps = ids.shape
    tokens = steps * batch

    def block_of(t, _, number, places):
        place = places[t % batch, t // batch] - number[0] * vocab_rows
        return (jnp.clip(place, 0, vocab_rows - 1) // 8, 0)

    return pl.pallas_call(
        functools.partial(pick_kernel, vocab_rows),
        out_shape=jax.ShapeDtypeStruct((chips, tokens, 128), BF16),
        grid_spec=pltpu.PrefetchScalarGridSpec(
            num_scalar_prefetch=2,
            grid=(1,),
            in_specs=[
                pl.BlockSpec((8, model_width), functools.partial(block_of, t))
                for t in range(tokens)
            ],
            out_specs=pl.BlockSpec((chips, tokens, 128), lambda _, number, places: (0, 0, 0)),
            scratch_shapes=[pltpu.VMEM((tokens, model_width), F32)],
        ),
        compiler_params=grant(50),
        name="pick",
    )(rank, ids, *([table] * tokens))


def joint_kernel(
    core, own, other, gain, weights, other_weights, out, stream_out, held, other_held, sems
):
    c = core[0]
    groups = ((0, Q_HALF), (HEADS, KV_HALF), (HEADS + KV_HEADS, KV_HALF))
    copies, at = [], 0
    for n, (first, count) in enumerate(groups):
        start = pl.multiple_of((first + count * c) * HEAD_DIM, HEAD_DIM)
        columns = pl.ds(start, count * HEAD_DIM)
        places = pl.ds(at * HEAD_DIM, count * HEAD_DIM)
        for side, (source, target) in enumerate(((weights, held), (other_weights, other_held))):
            copy = pltpu.make_async_copy(
                source.at[:, columns], target.at[:, places], sems.at[n, side]
            )
            copy.start()
            copies.append(copy)
        at += count
    width = gain.shape[1]
    features = width // 2
    both = own[...] + other[...]
    stream = both[:, :width]
    square = jnp.sum(both[:, width : width + 3], axis=-1, keepdims=True)
    normed = (stream * lax.rsqrt(square + NORM_EPS) * gain[...]).astype(BF16).astype(F32)
    stream_out[...] = stream
    mine, others = own_first(c, normed[:, :features], normed[:, features:])
    mine, others = mine.astype(BF16), others.astype(BF16)
    out[BLOCKS:] = jnp.zeros((out.shape[0] - BLOCKS, *out.shape[1:]), BF16)
    for copy in copies:
        copy.wait()
    product = jnp.dot(mine, held[...], preferred_element_type=F32)
    product += jnp.dot(others, other_held[...], preferred_element_type=F32)
    product = product.astype(BF16)
    for i in range(BLOCKS):
        out[i] = product[:, i * HEAD_DIM : (i + 1) * HEAD_DIM]


def rotate_kernel(place, got, bias, cosine, sine, out):
    total = jnp.sum(got[...].astype(F32), axis=0) + bias[pl.ds(place[0], 1), :]
    joint = total.astype(BF16).astype(F32)
    turned = joint * cosine[...] + pltpu.roll(joint, HALF, 1) * sine[...]
    result = jnp.where(place[1] > 0, turned, joint).astype(BF16)
    out[...] = jnp.broadcast_to(result[None], out.shape)


def attend_kernel(info, heads, keys, other_keys, values, other_values, out):
    tokens = heads.shape[1]
    batch, local_len, _ = keys.shape
    rows = GROUP * tokens
    score_scale = 1.0 / math.sqrt(HEAD_DIM)
    token = lax.broadcasted_iota(jnp.int32, (rows, 1), 0) % tokens
    prompt = token % batch
    spot = lax.broadcasted_iota(jnp.int32, (1, local_len), 1)
    fresh = lax.broadcasted_iota(jnp.int32, (1, tokens), 1)
    fresh_valid = (fresh % batch == prompt) & (fresh <= token) & (info[3] > 0)
    contract = (((1,), (1,)), ((), ()))
    lane = lanes((tokens, HEAD_DIM))
    valid = [
        [(spot + info[1 + side] < info[4 + b]) & (prompt == b) for b in range(batch)]
        for side in range(2)
    ]
    for h in range(KV_HALF):
        columns = slice(h * HEAD_DIM, (h + 1) * HEAD_DIM)
        query = heads[h * GROUP : (h + 1) * GROUP].astype(F32).reshape(rows, HEAD_DIM).astype(BF16)
        scores, kept, matching = [], [], []
        for side, (k_ref, v_ref) in enumerate(((keys, values), (other_keys, other_values))):
            for b in range(batch):
                score = lax.dot_general(
                    query, k_ref[b, :, columns], contract, preferred_element_type=F32
                )
                scores.append(jnp.where(valid[side][b], score * score_scale, MASKED))
                kept.append(valid[side][b])
                matching.append(v_ref[b, :, columns])
        score = lax.dot_general(
            query, heads[Q_HALF + h], contract, preferred_element_type=F32
        )
        scores.append(jnp.where(fresh_valid, score * score_scale, MASKED))
        kept.append(fresh_valid)
        matching.append(heads[Q_HALF + KV_HALF + h])
        top = functools.reduce(
            jnp.maximum, [jnp.max(s, axis=-1, keepdims=True) for s in scores]
        )
        total = jnp.zeros((rows, 1), F32)
        summed = jnp.zeros((rows, HEAD_DIM), F32)
        for s, keep, value in zip(scores, kept, matching):
            weight = jnp.where(keep, jnp.exp(s - top), 0.0)
            total += jnp.sum(weight, axis=-1, keepdims=True)
            summed += jnp.dot(weight.astype(BF16), value, preferred_element_type=F32)
        for g in range(GROUP):
            part = slice(g * tokens, (g + 1) * tokens)
            extra = jnp.zeros(lane.shape, F32)
            for i, piece in enumerate(in_pieces(top[part]) + in_pieces(total[part])):
                extra = jnp.where(lane == HALF + i, piece, extra)
            both = summed[part]
            at = 2 * (h * GROUP + g)
            out[at] = jnp.where(lane < HALF, both, extra).astype(BF16)
            out[at + 1] = jnp.where(lane < HALF, pltpu.roll(both, HALF, 1), extra).astype(BF16)
    used = 2 * Q_HALF
    out[used:] = jnp.zeros((out.shape[0] - used, *out.shape[1:]), BF16)


def attend(info, heads, keys, other_keys, values, other_values):
    batch, local_len, key_width = keys.shape
    cut = key_width // 2
    whole = pl.BlockSpec(heads.shape, lambda _, i: (0, 0, 0))
    mine = pl.BlockSpec((batch, local_len, cut), lambda _, i: (0, 0, i[0]))
    return pl.pallas_call(
        attend_kernel,
        out_shape=jax.ShapeDtypeStruct(heads.shape, BF16),
        grid_spec=pltpu.PrefetchScalarGridSpec(
            num_scalar_prefetch=1,
            grid=(1,),
            in_specs=[whole, mine, mine, mine, mine],
            out_specs=whole,
        ),
        compiler_params=grant(53),
        name="attend",
    )(info, heads, keys, other_keys, values, other_values)


def merge_kernel(got, out):
    parts = got[...].astype(F32)
    tops = jnp.sum(parts[:, :, HALF : HALF + 3], axis=-1, keepdims=True)
    scale = jnp.exp(tops - jnp.max(tops, axis=0, keepdims=True))
    merged = jnp.sum(parts * scale, axis=0)
    total = jnp.sum(merged[:, HALF + 3 : HALF + 6], axis=-1, keepdims=True)
    result = (merged / jnp.where(total > 0.0, total, 1.0)).astype(BF16)
    out[...] = jnp.broadcast_to(result[None], out.shape)


def project_kernel(
    core, own, other, weights, other_weights, stream, attended, mid_out, out, held, other_held, sems
):
    copies = [
        pltpu.make_async_copy(weights, held, sems.at[0]),
        pltpu.make_async_copy(other_weights, other_held, sems.at[1]),
    ]
    for copy in copies:
        copy.start()
    c = core[0]
    tokens, width = stream.shape
    lane = lanes((tokens, HEAD_DIM))
    for pieces, start in ((own, c * Q_HALF), (other, (1 - c) * Q_HALF)):
        for i in range(Q_HALF):
            low = pieces[2 * i].astype(F32)
            high = pltpu.roll(pieces[2 * i + 1].astype(F32), HALF, 1)
            column = pl.multiple_of((start + i) * HEAD_DIM, HEAD_DIM)
            attended[:, pl.ds(column, HEAD_DIM)] = jnp.where(lane < HALF, low, high).astype(BF16)
    rows = attended[...]
    contract = (((1,), (1,)), ((), ()))
    for copy in copies:
        copy.wait()
    mine = lax.dot_general(rows, held[...], contract, preferred_element_type=F32)
    others = lax.dot_general(rows, other_held[...], contract, preferred_element_type=F32)
    mid = stream[...] + jnp.concatenate(own_first(c, mine, others), axis=1)
    mid_out[...] = mid
    padded = jnp.concatenate([mid, jnp.zeros((tokens, HEAD_DIM - width), F32)], axis=1)
    out[...] = jnp.broadcast_to(padded.astype(BF16)[None], out.shape)


def mlp_kernel(got, gain, w_gate, w_up, w_down, out, flat, gate_held, up_held, down_held, sems):
    held = (gate_held, up_held, down_held)
    copies = [
        pltpu.make_async_copy(source, target, sems.at[n])
        for n, (source, target) in enumerate(zip((w_gate, w_up, w_down), held))
    ]
    for copy in copies:
        copy.start()
    chips, tokens, lane_count = got.shape
    model_width = flat.shape[1]
    width = model_width // chips
    parts = got[...].astype(F32)
    square = jnp.sum(jnp.sum(parts * parts, axis=0), axis=-1, keepdims=True) / model_width
    for j in range(chips):
        flat[:, j * width : (j + 1) * width] = parts[j, :, :width]
    normed = (flat[...] * lax.rsqrt(square + NORM_EPS) * gain[...]).astype(BF16)
    copies[0].wait()
    gate = jnp.dot(normed, gate_held[...], preferred_element_type=F32)
    copies[1].wait()
    upper = jnp.dot(normed, up_held[...], preferred_element_type=F32)
    hidden = (gate / (1.0 + jnp.exp(-gate)) * upper).astype(BF16)
    copies[2].wait()
    flat[...] = jnp.dot(hidden, down_held[...], preferred_element_type=F32)
    tail = jnp.zeros((tokens, lane_count - width), F32)
    for j in range(chips):
        both = jnp.concatenate([flat[:, j * width : (j + 1) * width], tail], axis=1)
        out[j] = both.astype(BF16)


def body(
    token_ids,
    lengths,
    embed_table,
    attn_gain,
    w_qkv,
    qkv_bias,
    cache_keys,
    cache_values,
    w_out,
    mlp_gain,
    w_gate,
    w_up,
    w_down,
):
    c = lax.axis_index(CORE)
    j = lax.axis_index(CHIPS)
    rank = lax.axis_index(SEQ)
    chips = lax.axis_size(CHIPS)
    steps, batch = token_ids.shape
    tokens = steps * batch
    model_width = embed_table.shape[1]
    local_len = cache_keys.shape[1]
    features = w_qkv.shape[0]
    width = 2 * features
    core = c.reshape(1)
    tile = (chips, tokens, HEAD_DIM)

    other_qkv = partner(w_qkv)
    other_keys = partner(cache_keys)
    other_values = partner(cache_values)
    own_out = w_out.T
    other_out = partner(own_out)

    sent = pick(rank.reshape(1), token_ids.T, embed_table, chips)
    got = jnp.sum(swap(sent).astype(F32), axis=0)
    gain = lax.dynamic_slice_in_dim(attn_gain, j * width, width, 0).astype(F32)[None]
    sent, stream = kernel_call(
        joint_kernel,
        (jax.ShapeDtypeStruct(tile, BF16), jax.ShapeDtypeStruct((tokens, width), F32)),
        [SCALARS] + [WHOLE] * 3 + [STAYS] * 2,
        [pltpu.VMEM((features, BLOCKS * HEAD_DIM), BF16)] * 2 + [pltpu.SemaphoreType.DMA((3, 2))],
        name="joint",
    )(core, got, partner(got), gain, w_qkv, other_qkv)

    positions = (lengths[None, :] + jnp.arange(steps, dtype=jnp.int32)[:, None]).reshape(-1)
    frequency = ROPE_BASE ** (-2.0 * jnp.arange(HALF, dtype=F32) / HEAD_DIM)
    angles = positions.astype(F32)[:, None] * frequency
    cosine = jnp.cos(angles)
    sine = jnp.sin(angles)
    cosine = jnp.concatenate([cosine, cosine], axis=1)
    sine = jnp.concatenate([-sine, sine], axis=1)
    head = jnp.where(
        j < Q_HALF,
        Q_HALF * c + j,
        jnp.where(
            j < Q_HALF + KV_HALF,
            HEADS + KV_HALF * c + (j - Q_HALF),
            HEADS + KV_HEADS + KV_HALF * c + (j - Q_HALF - KV_HALF),
        ),
    )
    head = jnp.where(j < BLOCKS, head, 0)
    place = jnp.stack([head, (j < Q_HALF + KV_HALF).astype(jnp.int32)])
    heads = kernel_call(
        rotate_kernel,
        jax.ShapeDtypeStruct(tile, BF16),
        [SCALARS] + [WHOLE] * 4,
        name="rotate",
    )(place, swap(sent), qkv_bias.reshape(-1, HEAD_DIM), cosine, sine)
    heads = swap(heads)

    info = jnp.stack(
        [
            c,
            rank * local_len,
            (rank + 1 - 2 * c) * local_len,
            (j == 0).astype(jnp.int32),
            *[lengths[b] for b in range(batch)],
        ]
    )
    partial = attend(info, heads, cache_keys, other_keys, cache_values, other_values)
    merged = kernel_call(merge_kernel, jax.ShapeDtypeStruct(tile, BF16), [WHOLE], name="merge")(
        swap(partial)
    )
    pieces = swap(merged)

    attended, mid, sent = kernel_call(
        project_kernel,
        (
            jax.ShapeDtypeStruct((tokens, HEADS * HEAD_DIM), BF16),
            jax.ShapeDtypeStruct((tokens, width), F32),
            jax.ShapeDtypeStruct(tile, BF16),
        ),
        [SCALARS] + [WHOLE] * 2 + [STAYS] * 2 + [WHOLE],
        [pltpu.VMEM(own_out.shape, BF16)] * 2 + [pltpu.SemaphoreType.DMA((2,))],
        name="project",
    )(core, pieces, partner(pieces), own_out, other_out, stream)

    down = kernel_call(
        mlp_kernel,
        jax.ShapeDtypeStruct(tile, BF16),
        [WHOLE] * 2 + [STAYS] * 3,
        [
            pltpu.VMEM((tokens, model_width), F32),
            *[pltpu.VMEM(weights.shape, BF16) for weights in (w_gate, w_up, w_down)],
            pltpu.SemaphoreType.DMA((3,)),
        ],
        name="mlp",
        room=53,
    )(swap(sent), mlp_gain.astype(F32)[None], w_gate, w_up, w_down)
    summed = jnp.sum(swap(down).astype(F32), axis=0)
    summed = mid + (summed + partner(summed))[:, :width]
    mine = jnp.where(c == 0, summed[:, :features], summed[:, features:])
    layer_out = mine.astype(BF16).reshape(steps, batch, features)
    return (attended.reshape(steps, batch, -1), layer_out)


def solution(mesh):
    finer = Mesh(
        mesh.devices.reshape(mesh.shape["parts"], 8, 8, 2), ("parts", "seq_0", "seq_1", "seq_2")
    )
    return jax.shard_map(
        body,
        mesh=finer,
        in_specs=(
            P(None, "parts"),
            P("parts"),
            P(SEQ, None),
            P(),
            P(SEQ, None),
            P(),
            P("parts", SEQ, None),
            P("parts", SEQ, None),
            P(None, SEQ),
            P(),
            P(None, SEQ),
            P(None, SEQ),
            P(SEQ, None),
        ),
        out_specs=(P(None, "parts", None), P(None, "parts", SEQ)),
        check_vma=False,
    )
```

```python
import functools
import math

import jax
import jax.numpy as jnp
from jax import lax
from jax.experimental import pallas as pl
from jax.experimental.pallas import tpu as pltpu
from jax.sharding import Mesh
from jax.sharding import PartitionSpec as P

HEADS = 40
KV_HEADS = 8
HEAD_DIM = 128
SEQ = ("seq_0", "seq_1", "seq_2")
CHIPS = ("seq_0", "seq_1")
CORE = "seq_2"

NORM_EPS = 1e-06
ROPE_BASE = 1000000.0
MASKED = -1e30
F32 = jnp.float32
BF16 = jnp.bfloat16
HALF = HEAD_DIM // 2
GROUP = HEADS // KV_HEADS
KV_HALF = KV_HEADS // 2
Q_HALF = HEADS // 2
BLOCKS = Q_HALF + 2 * KV_HALF

WHOLE = pl.BlockSpec(memory_space=pltpu.VMEM)
SCALARS = pl.BlockSpec(memory_space=pltpu.SMEM)
STAYS = pl.BlockSpec(memory_space=pltpu.HBM)


def grant(mebibytes):
    return pltpu.CompilerParams(vmem_limit_bytes=mebibytes * 1024 * 1024)


def kernel_call(body, out_shape, in_specs, scratch=(), name=None, room=12):
    many = isinstance(out_shape, (tuple, list))
    return pl.pallas_call(
        body,
        out_shape=out_shape,
        in_specs=in_specs,
        out_specs=[WHOLE] * len(out_shape) if many else WHOLE,
        scratch_shapes=list(scratch),
        compiler_params=grant(room),
        name=name,
    )


def swap(parts):
    return lax.all_to_all(parts, CHIPS, 0, 0)


def partner(array):
    return lax.ppermute(array, CORE, [(0, 1), (1, 0)])


def lanes(shape):
    return lax.broadcasted_iota(jnp.int32, shape, len(shape) - 1)


def in_pieces(value):
    high = value.astype(BF16).astype(F32)
    rest = value - high
    middle = rest.astype(BF16).astype(F32)
    return high, middle, rest - middle


def own_first(core, left, right):
    return jnp.where(core == 0, left, right), jnp.where(core == 0, right, left)


def pick_kernel(vocab_rows, rank, ids, *refs):
    tokens = len(refs) - 2
    batch = ids.shape[0]
    blocks, out, rows = refs[:tokens], refs[tokens], refs[tokens + 1]
    chips, _, lane_count = out.shape
    model_width = rows.shape[1]
    width = model_width // chips
    for t in range(tokens):
        place = ids[t % batch, t // batch] - rank[0] * vocab_rows
        inside = (place >= 0) & (place < vocab_rows)
        row = jnp.where(inside, place & 7, -1)
        block = blocks[t][...].astype(F32)
        at = lax.broadcasted_iota(jnp.int32, block.shape, 0)
        rows[t : t + 1, :] = jnp.sum(jnp.where(at == row, block, 0.0), axis=0, keepdims=True)
    values = rows[...]
    square = in_pieces(jnp.mean(values * values, axis=-1, keepdims=True))
    lane = lanes((tokens, lane_count - width))
    tail = jnp.zeros(lane.shape, F32)
    for i, piece in enumerate(square):
        tail = jnp.where(lane == i, piece, tail)
    for j in range(chips):
        both = jnp.concatenate([rows[:, j * width : (j + 1) * width], tail], axis=1)
        out[j] = both.astype(BF16)


def pick(rank, ids, table, chips):
    vocab_rows, model_width = table.shape
    batch, steps = ids.shape
    tokens = steps * batch

    def block_of(t, _, number, places):
        place = places[t % batch, t // batch] - number[0] * vocab_rows
        return (jnp.clip(place, 0, vocab_rows - 1) // 8, 0)

    return pl.pallas_call(
        functools.partial(pick_kernel, vocab_rows),
        out_shape=jax.ShapeDtypeStruct((chips, tokens, 128), BF16),
        grid_spec=pltpu.PrefetchScalarGridSpec(
            num_scalar_prefetch=2,
            grid=(1,),
            in_specs=[
                pl.BlockSpec((8, model_width), functools.partial(block_of, t))
                for t in range(tokens)
            ],
            out_specs=pl.BlockSpec((chips, tokens, 128), lambda _, number, places: (0, 0, 0)),
            scratch_shapes=[pltpu.VMEM((tokens, model_width), F32)],
        ),
        compiler_params=grant(50),
        name="pick",
    )(rank, ids, *([table] * tokens))


def joint_kernel(
    core, own, other, gain, weights, other_weights, out, stream_out, held, other_held, sems
):
    c = core[0]
    groups = ((0, Q_HALF), (HEADS, KV_HALF), (HEADS + KV_HEADS, KV_HALF))
    copies, at = [], 0
    for n, (first, count) in enumerate(groups):
        start = pl.multiple_of((first + count * c) * HEAD_DIM, HEAD_DIM)
        columns = pl.ds(start, count * HEAD_DIM)
        places = pl.ds(at * HEAD_DIM, count * HEAD_DIM)
        for side, (source, target) in enumerate(((weights, held), (other_weights, other_held))):
            copy = pltpu.make_async_copy(
                source.at[:, columns], target.at[:, places], sems.at[n, side]
            )
            copy.start()
            copies.append(copy)
        at += count
    width = gain.shape[1]
    features = width // 2
    both = own[...] + other[...]
    stream = both[:, :width]
    square = jnp.sum(both[:, width : width + 3], axis=-1, keepdims=True)
    normed = (stream * lax.rsqrt(square + NORM_EPS) * gain[...]).astype(BF16).astype(F32)
    stream_out[...] = stream
    mine, others = own_first(c, normed[:, :features], normed[:, features:])
    mine, others = mine.astype(BF16), others.astype(BF16)
    out[BLOCKS:] = jnp.zeros((out.shape[0] - BLOCKS, *out.shape[1:]), BF16)
    for copy in copies:
        copy.wait()
    product = jnp.dot(mine, held[...], preferred_element_type=F32)
    product += jnp.dot(others, other_held[...], preferred_element_type=F32)
    product = product.astype(BF16)
    for i in range(BLOCKS):
        out[i] = product[:, i * HEAD_DIM : (i + 1) * HEAD_DIM]


def rotate_kernel(place, got, bias, cosine, sine, out):
    total = jnp.sum(got[...].astype(F32), axis=0) + bias[pl.ds(place[0], 1), :]
    joint = total.astype(BF16).astype(F32)
    turned = joint * cosine[...] + pltpu.roll(joint, HALF, 1) * sine[...]
    result = jnp.where(place[1] > 0, turned, joint).astype(BF16)
    out[...] = jnp.broadcast_to(result[None], out.shape)


def attend_kernel(
    info, heads, keys, other_keys, values, other_values, out, key_parts, value_parts, sems
):
    tokens = heads.shape[1]
    _, batch, local_len, cut = key_parts.shape
    columns = pl.ds(pl.multiple_of(info[0] * cut, cut), cut)
    copies = []
    for n, (mine, others, parts) in enumerate(
        ((keys, other_keys, key_parts), (values, other_values, value_parts))
    ):
        for side, source in enumerate((mine, others)):
            copy = pltpu.make_async_copy(
                source.at[:, :, columns], parts.at[side], sems.at[n, side]
            )
            copy.start()
            copies.append(copy)
    rows = GROUP * tokens
    score_scale = 1.0 / math.sqrt(HEAD_DIM)
    token = lax.broadcasted_iota(jnp.int32, (rows, 1), 0) % tokens
    prompt = token % batch
    spot = lax.broadcasted_iota(jnp.int32, (1, local_len), 1)
    fresh = lax.broadcasted_iota(jnp.int32, (1, tokens), 1)
    fresh_valid = (fresh % batch == prompt) & (fresh <= token) & (info[3] > 0)
    fresh_mask = jnp.where(fresh_valid, 0.0, MASKED)
    chunks = [(side, b) for side in range(2) for b in range(batch)]
    mask = jnp.concatenate(
        [
            jnp.where((spot + info[1 + side] < info[4 + b]) & (prompt == b), 0.0, MASKED)
            for side, b in chunks
        ],
        axis=1,
    )
    contract = (((1,), (1,)), ((), ()))
    lane = lanes((tokens, HEAD_DIM))
    used = 2 * Q_HALF
    out[used:] = jnp.zeros((out.shape[0] - used, *out.shape[1:]), BF16)
    places = [slice(h * HEAD_DIM, (h + 1) * HEAD_DIM) for h in range(KV_HALF)]
    queries = [
        heads[h * GROUP : (h + 1) * GROUP].astype(F32).reshape(rows, HEAD_DIM).astype(BF16)
        for h in range(KV_HALF)
    ]
    fresh_scores = [
        lax.dot_general(queries[h], heads[Q_HALF + h], contract, preferred_element_type=F32)
        * score_scale
        + fresh_mask
        for h in range(KV_HALF)
    ]
    copies[0].wait()
    copies[1].wait()
    scores = []
    for h in range(KV_HALF):
        found = [
            lax.dot_general(
                queries[h], key_parts[side, b, :, places[h]], contract, preferred_element_type=F32
            )
            for side, b in chunks
        ]
        scores.append(jnp.concatenate(found, axis=1) * score_scale + mask)
    tops = [
        jnp.maximum(
            jnp.maximum(
                jnp.max(scores[h], axis=-1, keepdims=True),
                jnp.max(fresh_scores[h], axis=-1, keepdims=True),
            ),
            0.1 * MASKED,
        )
        for h in range(KV_HALF)
    ]
    weights = [jnp.exp(scores[h] - tops[h]) for h in range(KV_HALF)]
    fresh_weights = [jnp.exp(fresh_scores[h] - tops[h]) for h in range(KV_HALF)]
    totals = [
        jnp.sum(weights[h], axis=-1, keepdims=True)
        + jnp.sum(fresh_weights[h], axis=-1, keepdims=True)
        for h in range(KV_HALF)
    ]
    weights = [weight.astype(BF16) for weight in weights]
    copies[2].wait()
    copies[3].wait()
    for h in range(KV_HALF):
        summed = jnp.dot(
            fresh_weights[h].astype(BF16),
            heads[Q_HALF + KV_HALF + h],
            preferred_element_type=F32,
        )
        for n, (side, b) in enumerate(chunks):
            summed += jnp.dot(
                weights[h][:, n * local_len : (n + 1) * local_len],
                value_parts[side, b, :, places[h]],
                preferred_element_type=F32,
            )
        for g in range(GROUP):
            part = slice(g * tokens, (g + 1) * tokens)
            extra = jnp.zeros(lane.shape, F32)
            for i, piece in enumerate(in_pieces(tops[h][part]) + in_pieces(totals[h][part])):
                extra = jnp.where(lane == HALF + i, piece, extra)
            both = summed[part]
            at = 2 * (h * GROUP + g)
            out[at] = jnp.where(lane < HALF, both, extra).astype(BF16)
            out[at + 1] = jnp.where(lane < HALF, pltpu.roll(both, HALF, 1), extra).astype(BF16)


def merge_kernel(got, out):
    parts = got[...].astype(F32)
    tops = jnp.sum(parts[:, :, HALF : HALF + 3], axis=-1, keepdims=True)
    scale = jnp.exp(tops - jnp.max(tops, axis=0, keepdims=True))
    merged = jnp.sum(parts * scale, axis=0)
    total = jnp.sum(merged[:, HALF + 3 : HALF + 6], axis=-1, keepdims=True)
    result = (merged / jnp.where(total > 0.0, total, 1.0)).astype(BF16)
    out[...] = jnp.broadcast_to(result[None], out.shape)


def project_kernel(
    core,
    own,
    other,
    weights,
    other_weights,
    stream,
    attended,
    mid_out,
    out,
    rows_held,
    held,
    other_held,
    sems,
):
    copies = [
        pltpu.make_async_copy(weights, held, sems.at[0]),
        pltpu.make_async_copy(other_weights, other_held, sems.at[1]),
    ]
    for copy in copies:
        copy.start()
    c = core[0]
    tokens, width = stream.shape
    lane = lanes((tokens, HEAD_DIM))
    for pieces, start in ((own, c * Q_HALF), (other, (1 - c) * Q_HALF)):
        for i in range(Q_HALF):
            low = pieces[2 * i].astype(F32)
            high = pltpu.roll(pieces[2 * i + 1].astype(F32), HALF, 1)
            column = pl.multiple_of((start + i) * HEAD_DIM, HEAD_DIM)
            both = jnp.where(lane < HALF, low, high).astype(BF16)
            rows_held[:, pl.ds(column, HEAD_DIM)] = both
    rows = rows_held[...]
    steps, batch, _ = attended.shape
    for step in range(steps):
        attended[step] = rows[step * batch : (step + 1) * batch]
    contract = (((1,), (1,)), ((), ()))
    for copy in copies:
        copy.wait()
    mine = lax.dot_general(rows, held[...], contract, preferred_element_type=F32)
    others = lax.dot_general(rows, other_held[...], contract, preferred_element_type=F32)
    mid = stream[...] + jnp.concatenate(own_first(c, mine, others), axis=1)
    mid_out[...] = mid
    padded = jnp.concatenate([mid, jnp.zeros((tokens, HEAD_DIM - width), F32)], axis=1)
    out[...] = jnp.broadcast_to(padded.astype(BF16)[None], out.shape)


def mlp_kernel(got, gain, w_gate, w_up, w_down, out, flat, gate_held, up_held, down_held, sems):
    held = (gate_held, up_held, down_held)
    copies = [
        pltpu.make_async_copy(source, target, sems.at[n])
        for n, (source, target) in enumerate(zip((w_gate, w_up, w_down), held))
    ]
    for copy in copies:
        copy.start()
    chips, tokens, lane_count = got.shape
    model_width = flat.shape[1]
    width = model_width // chips
    parts = got[...].astype(F32)
    square = jnp.sum(jnp.sum(parts * parts, axis=0), axis=-1, keepdims=True) / model_width
    for j in range(chips):
        flat[:, j * width : (j + 1) * width] = parts[j, :, :width]
    normed = (flat[...] * lax.rsqrt(square + NORM_EPS) * gain[...]).astype(BF16)
    copies[0].wait()
    gate = jnp.dot(normed, gate_held[...], preferred_element_type=F32)
    copies[1].wait()
    upper = jnp.dot(normed, up_held[...], preferred_element_type=F32)
    hidden = (gate / (1.0 + jnp.exp(-gate)) * upper).astype(BF16)
    copies[2].wait()
    flat[...] = jnp.dot(hidden, down_held[...], preferred_element_type=F32)
    tail = jnp.zeros((tokens, lane_count - width), F32)
    for j in range(chips):
        both = jnp.concatenate([flat[:, j * width : (j + 1) * width], tail], axis=1)
        out[j] = both.astype(BF16)


def body(
    token_ids,
    lengths,
    embed_table,
    attn_gain,
    w_qkv,
    qkv_bias,
    cache_keys,
    cache_values,
    w_out,
    mlp_gain,
    w_gate,
    w_up,
    w_down,
):
    c = lax.axis_index(CORE)
    j = lax.axis_index(CHIPS)
    rank = lax.axis_index(SEQ)
    chips = lax.axis_size(CHIPS)
    steps, batch = token_ids.shape
    tokens = steps * batch
    model_width = embed_table.shape[1]
    local_len = cache_keys.shape[1]
    features = w_qkv.shape[0]
    width = 2 * features
    core = c.reshape(1)
    tile = (chips, tokens, HEAD_DIM)

    other_qkv = partner(w_qkv)
    other_keys = partner(cache_keys)
    other_values = partner(cache_values)
    own_out = w_out.T
    other_out = partner(own_out)

    positions = (lengths[None, :] + jnp.arange(steps, dtype=jnp.int32)[:, None]).reshape(-1)
    frequency = ROPE_BASE ** (-2.0 * jnp.arange(HALF, dtype=F32) / HEAD_DIM)
    angles = positions.astype(F32)[:, None] * frequency
    cosine = jnp.cos(angles)
    sine = jnp.sin(angles)
    cosine = jnp.concatenate([cosine, cosine], axis=1)
    sine = jnp.concatenate([-sine, sine], axis=1)
    head = jnp.where(
        j < Q_HALF,
        Q_HALF * c + j,
        jnp.where(
            j < Q_HALF + KV_HALF,
            HEADS + KV_HALF * c + (j - Q_HALF),
            HEADS + KV_HEADS + KV_HALF * c + (j - Q_HALF - KV_HALF),
        ),
    )
    head = jnp.where(j < BLOCKS, head, 0)
    place = jnp.stack([head, (j < Q_HALF + KV_HALF).astype(jnp.int32)])
    info = jnp.stack(
        [
            c,
            rank * local_len,
            (rank + 1 - 2 * c) * local_len,
            (j == 0).astype(jnp.int32),
            *[lengths[b] for b in range(batch)],
        ]
    )
    sent = pick(rank.reshape(1), token_ids.T, embed_table, chips)
    got = jnp.sum(swap(sent).astype(F32), axis=0)
    gain = lax.dynamic_slice_in_dim(attn_gain, j * width, width, 0).astype(F32)[None]
    sent, stream = kernel_call(
        joint_kernel,
        (jax.ShapeDtypeStruct(tile, BF16), jax.ShapeDtypeStruct((tokens, width), F32)),
        [SCALARS] + [WHOLE] * 3 + [STAYS] * 2,
        [pltpu.VMEM((features, BLOCKS * HEAD_DIM), BF16)] * 2 + [pltpu.SemaphoreType.DMA((3, 2))],
        name="joint",
    )(core, got, partner(got), gain, w_qkv, other_qkv)

    sent, place, cosine, sine, info, bias, mlp_gain, other_keys, other_values, other_out = (
        lax.optimization_barrier(
            (
                sent,
                place,
                cosine,
                sine,
                info,
                qkv_bias.reshape(-1, HEAD_DIM),
                mlp_gain.astype(F32)[None],
                other_keys,
                other_values,
                other_out,
            )
        )
    )

    heads = kernel_call(
        rotate_kernel,
        jax.ShapeDtypeStruct(tile, BF16),
        [SCALARS] + [WHOLE] * 4,
        name="rotate",
    )(place, swap(sent), bias, cosine, sine)
    heads = swap(heads)

    parts = (2, batch, local_len, KV_HALF * HEAD_DIM)
    partial = kernel_call(
        attend_kernel,
        jax.ShapeDtypeStruct(tile, BF16),
        [SCALARS, WHOLE] + [STAYS] * 4,
        [pltpu.VMEM(parts, BF16)] * 2 + [pltpu.SemaphoreType.DMA((2, 2))],
        name="attend",
        room=53,
    )(info, heads, cache_keys, other_keys, cache_values, other_values)
    merged = kernel_call(merge_kernel, jax.ShapeDtypeStruct(tile, BF16), [WHOLE], name="merge")(
        swap(partial)
    )
    pieces = swap(merged)

    attended, mid, sent = kernel_call(
        project_kernel,
        (
            jax.ShapeDtypeStruct((steps, batch, HEADS * HEAD_DIM), BF16),
            jax.ShapeDtypeStruct((tokens, width), F32),
            jax.ShapeDtypeStruct(tile, BF16),
        ),
        [SCALARS] + [WHOLE] * 2 + [STAYS] * 2 + [WHOLE],
        [pltpu.VMEM((tokens, HEADS * HEAD_DIM), BF16)]
        + [pltpu.VMEM(own_out.shape, BF16)] * 2
        + [pltpu.SemaphoreType.DMA((2,))],
        name="project",
    )(core, pieces, partner(pieces), own_out, other_out, stream)

    down = kernel_call(
        mlp_kernel,
        jax.ShapeDtypeStruct(tile, BF16),
        [WHOLE] * 2 + [STAYS] * 3,
        [
            pltpu.VMEM((tokens, model_width), F32),
            *[pltpu.VMEM(weights.shape, BF16) for weights in (w_gate, w_up, w_down)],
            pltpu.SemaphoreType.DMA((3,)),
        ],
        name="mlp",
        room=53,
    )(swap(sent), mlp_gain, w_gate, w_up, w_down)
    summed = jnp.sum(swap(down).astype(F32), axis=0)
    summed = mid + (summed + partner(summed))[:, :width]
    mine = jnp.where(c == 0, summed[:, :features], summed[:, features:])
    layer_out = mine.astype(BF16).reshape(steps, batch, features)
    return (attended, layer_out)


def solution(mesh):
    finer = Mesh(
        mesh.devices.reshape(mesh.shape["parts"], 8, 8, 2), ("parts", "seq_0", "seq_1", "seq_2")
    )
    return jax.shard_map(
        body,
        mesh=finer,
        in_specs=(
            P(None, "parts"),
            P("parts"),
            P(SEQ, None),
            P(),
            P(SEQ, None),
            P(),
            P("parts", SEQ, None),
            P("parts", SEQ, None),
            P(None, SEQ),
            P(),
            P(None, SEQ),
            P(None, SEQ),
            P(SEQ, None),
        ),
        out_specs=(P(None, "parts", None), P(None, "parts", SEQ)),
        check_vma=False,
    )
```
